32 devices in a mesh: expert: 8 (over z, y), half: 4 (over x, core).
Axes of the slice: x: 2, y: 2, z: 4, core: 2. Of those that a mesh axis runs over, the one named last changes fastest.
Arguments:
- tokens: bfloat16 [1024, 2048], P('expert', 'half'), may hold values from -6 to 6
- cotangent: bfloat16 [1024, 2048], P('expert', 'half'), may hold values from -4 to 4
- route: int32 [1024, 8], P('expert'), may hold values from 0 to 15, all different within a row; in each aligned block of 128 rows (0 to 127, 128 to 255, ...) at most 128 rows name the same one
- prob: bfloat16 [1024, 8], P('expert'), may hold values from 0.19921875 to 1
- w_gate: bfloat16 [16, 768, 2048], P('expert', 'half'), may hold values from -0.125 to 0.125
- w_up: bfloat16 [16, 768, 2048], P('expert', 'half'), may hold values from -0.125 to 0.125
- w_down: bfloat16 [16, 768, 2048], P('expert', 'half'), may hold values from -0.21875 to 0.21875
Outputs:
- grad_tokens: bfloat16 [1024, 2048], P('expert', 'half')
- grad_prob: float32 [1024, 8], P('expert')
- grad_gate: bfloat16 [16, 768, 2048], P('expert', 'half')
- grad_up: bfloat16 [16, 768, 2048], P('expert', 'half')
- grad_down: bfloat16 [16, 768, 2048], P('expert', 'half')
The draws below stay inside these ranges and needn't reach their ends.
Inputs may be any that keep to these rules, and one draw needn't show every extreme that they name: `route`: each row names 8 different experts; among the rows of one device no expert is named more than 128 times, and that most is reached.
All inputs are finite; a program needn't handle non-finite values.
Results may differ from the reference program's by a relative error of at most 0.013.
Values may be sent and summed in bfloat16 or wider, within the bound.
A program may use at most 192 MiB of HBM per device.

```python
import math
import jax
import jax.numpy as jnp
import numpy as np
from jax import lax

D = 2048
FF = 768
K = 8
TOK_DEV = 128
E = 16
TOKENS = 1024
CAP = 128
N_EXPERT = 8
N_HALF = 4


def block_levels(key, extent, split, smallest, top_value):
    loudness, own = 1.0, jax.random.fold_in(key, 6)
    for position, blocks in split:
        steps = jnp.exp(jax.random.uniform(jax.random.fold_in(own, position), (blocks,), jnp.float32, smallest / len(split), top_value / len(split)))
        loudness = loudness * jnp.repeat(steps, extent[position] // blocks).reshape([-1 if axis == position else 1 for axis in range(len(extent))])
    return loudness


def shared_out(key, own, number, rows, number_of, top, limit, lean):
    order = jax.random.permutation(key, number_of)
    packed, usual = load_shares(number_of, rows * top, limit, lean, True), load_shares(number_of, rows * top, limit, lean, False)
    places = jnp.arange(number_of)

    def named(sizes, offset_by):
        used = int((sizes > 0).sum())
        fixed = max(1, used // 4)
        shifted = fixed + (places - fixed + offset_by * (used - fixed)) % max(1, number_of - fixed)
        return jnp.zeros((number_of,), jnp.int32).at[order[jnp.where(places < fixed, places, shifted)]].set(jnp.asarray(sizes, jnp.int32))

    sizes = jnp.where(number % 4 == 0, named(packed, number // 4), named(usual, number - number // 4 - 1))
    mixed = jax.random.permutation(jax.random.fold_in(own, 3), number_of)
    giver, sink = mixed[0:number_of // 2 * 2:2], mixed[1:number_of // 2 * 2:2]
    margin = jnp.minimum(sizes[giver] - 1, limit - sizes[sink]) // 2
    margin = jnp.where((giver == order[0]) | (sink == order[0]) | (sizes[sink] == 0), 0, jnp.maximum(margin, 0))
    shifted = jax.random.randint(jax.random.fold_in(own, 4), (number_of // 2,), 0, 1 << 20) % (margin + 1)
    sizes = sizes.at[giver].add(-shifted).at[sink].add(shifted)
    members = jnp.searchsorted(jnp.cumsum(sizes), jnp.arange(rows * top), side="right").astype(jnp.int32)
    table = members.reshape(top, rows).T
    table = table[jax.random.permutation(jax.random.fold_in(own, 1), rows)]
    offset_by = jax.random.randint(jax.random.fold_in(own, 2), (rows, 1), 0, top)
    return jnp.take_along_axis(table, (jnp.arange(top)[None, :] + offset_by) % top, axis=1)


def load_shares(number_of, total, reach, skew, full):
    loads = [(1 << 20) // math.isqrt(rank ** skew) + 1 for rank in range(1, number_of + 1)]
    largest = reach if full else min(reach, max(-(-total // number_of), total * loads[0] // sum(loads)))
    least = 1 if total - largest >= number_of - 1 else 0
    counts, rest = [largest] + [least] * (number_of - 1), total - largest - least * (number_of - 1)
    while rest > 0:
        movable = [i for i in range(1, number_of) if counts[i] < largest] or [i for i in range(1, number_of) if counts[i] < reach]
        whole, budget = sum([loads[i] for i in movable]), rest
        for i in movable:
            more = min(reach - counts[i], max(1, budget * loads[i] // whole), rest)
            counts[i] = counts[i] + more
            rest = rest - more
    return np.array(counts)


def bell_draw(rng, shape, scale, bound, split=(), kind=jnp.bfloat16):
    array = scale * jax.random.normal(rng, shape, jnp.float32)
    if split:
        array = array * block_levels(rng, shape, split, -0.22, 0.18)
    return jnp.clip(array, -bound, bound).astype(kind)


def setup_inputs(seed: int = 0) -> dict:
    key_of = jax.random.split(jax.random.key(seed), 8)
    tokens = bell_draw(key_of[0], (TOKENS, D), 1.0, 6.0, ((0, 8), (1, 4)))
    cotangent = bell_draw(key_of[1], (TOKENS, D), 0.5, 4.0, ((0, 8), (1, 4)))
    route_keys = jax.random.split(jax.random.fold_in(key_of[2], 1), TOKENS // TOK_DEV)
    route_turns = jax.random.permutation(jax.random.fold_in(key_of[2], 3), TOKENS // TOK_DEV)
    route = jax.vmap(lambda own, number: shared_out(jax.random.fold_in(key_of[2], 2), own, number, TOK_DEV, E, K, CAP, 2))(route_keys, route_turns).reshape((TOKENS, K))
    prob = jnp.clip(0.19921875 + 0.80078125 * jax.random.uniform(key_of[3], (TOKENS, K), jnp.float32) ** block_levels(key_of[3], (TOKENS, K), ((0, 8),), -0.2, 0.2), 0.19921875, 1.0).astype(jnp.bfloat16)
    w_gate = bell_draw(key_of[4], (E, FF, D), D ** -0.5, 0.125, ((0, 8), (1, 4)))
    w_up = bell_draw(key_of[5], (E, FF, D), D ** -0.5, 0.125, ((0, 8), (1, 4)))
    w_down = bell_draw(key_of[6], (E, FF, D), FF ** -0.5, 0.21875, ((0, 8), (1, 4)))
    return dict(tokens=tokens, cotangent=cotangent, route=route, prob=prob, w_gate=w_gate, w_up=w_up, w_down=w_down)


def reference(tokens, cotangent, route, prob, w_gate, w_up, w_down):
    flat_route = route.reshape(-1)
    flat_prob = prob.reshape(-1).astype(jnp.float32)
    rows_max = N_EXPERT * CAP
    count = TOKENS * K
    order = jnp.arange(count, dtype=jnp.int32)
    quarter = FF // N_HALF

    def one_expert(carry, expert):
        grad_in, grad_weight = carry
        chosen = flat_route == expert
        place = jnp.where(chosen, jnp.cumsum(chosen.astype(jnp.int32)) - 1, rows_max).astype(jnp.int32)
        source = jnp.zeros((rows_max,), jnp.int32).at[place].set(order, mode="drop")
        filled = jnp.zeros((rows_max,), jnp.float32).at[place].set(1.0, mode="drop")
        token_of = (source // K).astype(jnp.int32)
        keep = filled[:, None] > 0.5
        xin = jnp.where(keep, tokens[token_of], jnp.zeros((), jnp.bfloat16))
        dout = jnp.where(keep, cotangent[token_of], jnp.zeros((), jnp.bfloat16))
        weight = flat_prob[source] * filled
        wgate = w_gate[expert]
        wup = w_up[expert]
        wdown = w_down[expert]
        gate = jnp.dot(xin, wgate.T, preferred_element_type=jnp.float32)
        upval = jnp.dot(xin, wup.T, preferred_element_type=jnp.float32)
        sig = jax.nn.sigmoid(gate)
        act = gate * sig
        hidden = (act * upval).astype(jnp.bfloat16)
        raw = jnp.dot(dout, wdown.T, preferred_element_type=jnp.float32)
        score = jnp.sum(hidden.astype(jnp.float32) * raw, axis=1)
        scaled = (weight[:, None] * dout.astype(jnp.float32)).astype(jnp.bfloat16)
        dact = weight[:, None] * raw
        dgate = (dact * upval * sig * (1.0 + gate * (1.0 - sig))).astype(jnp.bfloat16)
        dup = (dact * act).astype(jnp.bfloat16)
        grad_down = jnp.dot(hidden.T, scaled, preferred_element_type=jnp.float32).astype(jnp.bfloat16)
        grad_gate = jnp.dot(dgate.T, xin, preferred_element_type=jnp.float32).astype(jnp.bfloat16)
        grad_up = jnp.dot(dup.T, xin, preferred_element_type=jnp.float32).astype(jnp.bfloat16)
        dgate_f = dgate.astype(jnp.float32).reshape(rows_max, N_HALF, quarter)
        dup_f = dup.astype(jnp.float32).reshape(rows_max, N_HALF, quarter)
        wgate_f = wgate.astype(jnp.float32).reshape(N_HALF, quarter, D)
        wup_f = wup.astype(jnp.float32).reshape(N_HALF, quarter, D)
        parts = jnp.einsum("rhf,hfd->hrd", dgate_f, wgate_f) + jnp.einsum("rhf,hfd->hrd", dup_f, wup_f)
        parts = parts.astype(jnp.bfloat16).astype(jnp.float32)
        part_sum = jnp.sum(parts, axis=0) * filled[:, None]
        grad_in = grad_in.at[token_of].add(part_sum)
        grad_weight = grad_weight.at[source].add(score * filled)
        return (grad_in, grad_weight), (grad_gate, grad_up, grad_down)

    start = (jnp.zeros((TOKENS, D), jnp.float32), jnp.zeros((count,), jnp.float32))
    (grad_in, grad_weight), (grad_gate, grad_up, grad_down) = lax.scan(one_expert, start, jnp.arange(E, dtype=jnp.int32))
    return grad_in.astype(jnp.bfloat16), grad_weight.reshape(TOKENS, K), grad_gate, grad_up, grad_down
```

```python
import functools

import jax
import jax.numpy as jnp
from jax import lax
from jax.experimental import pallas as pl
from jax.experimental.pallas import tpu as pltpu
from jax.sharding import PartitionSpec as P

BOTH = ("expert", "half")


def gather_all(block, groups, halves):
    rows, quarter = block.shape
    parts = lax.all_gather(block, BOTH, axis=0).reshape(groups, halves, rows, quarter)
    return parts.transpose(0, 2, 1, 3).reshape(groups * rows, halves * quarter)


LANES = 128
MESH = pl.DeviceIdType.MESH


def place(groups):
    e, h = lax.axis_index("expert"), lax.axis_index("half")
    return lax.div(e, 2), lax.rem(e, 2), lax.div(h, 2), lax.rem(h, 2)


def greet(peers):
    barrier = pltpu.get_barrier_semaphore()
    for peer in peers:
        pl.semaphore_signal(barrier, inc=1, device_id=peer, device_id_type=MESH)
    pl.semaphore_wait(barrier, len(peers))


def gather_kernel(
    groups, tok_ref, cot_ref, tab_ref, x_ref, d_ref, w_ref,
    send_sem, z_sem, p_sem, q_sem, c_sem, tab_send, tab_recv, own_sem,
):
    line = groups // 2
    z, y, x, c = place(groups)
    e, h = 2 * z + y, 2 * x + c
    rows, quarter = tok_ref.shape
    y_peer = (2 * z + 1 - y, h)
    x_peer = (e, 2 * (1 - x) + c)
    c_peer = (e, 2 * x + 1 - c)
    ring = [(lax.rem(e + s, groups), h) for s in range(1, groups)]
    greet(ring + [x_peer, c_peer])

    sends, owns = [], []

    def push(src, dst, peer, number, sem):
        copy = pltpu.make_async_remote_copy(
            src_ref=src, dst_ref=dst, send_sem=number, recv_sem=sem,
            device_id=peer, device_id_type=MESH,
        )
        copy.start()
        sends.append(copy)

    def slot(out, zz, yy, xx, cc):
        row = pl.multiple_of((2 * zz + yy) * rows, rows)
        col = pl.multiple_of((2 * xx + cc) * quarter, quarter)
        return out.at[pl.ds(row, rows), pl.ds(col, quarter)]

    arrays = []
    for a, (src, out) in enumerate(((tok_ref, x_ref), (cot_ref, d_ref))):
        first, second = (y_peer, x_peer) if a == 0 else (x_peer, y_peer)

        def at(step, kind, out=out, a=a):
            zz = lax.rem(z - step + line, line)
            flip_first, flip_second = kind % 2, kind // 2
            fy, fx = (flip_first, flip_second) if a == 0 else (flip_second, flip_first)
            return slot(out, zz, 1 - y if fy else y, 1 - x if fx else x, c)

        arrays.append((a, src, out, first, second, at))

    def wait(a, at, step, kind, sem):
        here = at(step, kind)
        pltpu.make_async_remote_copy(
            src_ref=here, dst_ref=here, send_sem=own_sem.at[a], recv_sem=sem,
            device_id=c_peer, device_id_type=MESH,
        ).wait_recv()

    for a, src, out, first, second, at in arrays:
        here = slot(out, z, y, x, c)
        for s in range(1, line):
            push(src, here, (2 * lax.rem(z + s, line) + y, h), send_sem.at[a, s - 1], z_sem.at[a, s])
        own = pltpu.make_async_copy(src, here, own_sem.at[a])
        own.start()
        owns.append(own)
    for s in range(1, groups):
        here = w_ref.at[pl.ds(pl.multiple_of(e * rows, rows), rows), :]
        push(tab_ref, here, ring[s - 1], tab_send.at[s], tab_recv.at[s])
    own = pltpu.make_async_copy(
        tab_ref, w_ref.at[pl.ds(pl.multiple_of(e * rows, rows), rows), :], own_sem.at[2]
    )
    own.start()
    owns.append(own)

    base = line - 1
    for s in range(line + 2):
        for a, src, out, first, second, at in arrays:
            if s < line:
                if s > 0:
                    wait(a, at, s, 0, z_sem.at[a, s])
                there = at(s, 0)
                have = src if s == 0 else there
                push(have, there, first, send_sem.at[a, base + s], p_sem.at[a, s])
                push(have, there, second, send_sem.at[a, base + line + s], q_sem.at[a, s])
                push(have, there, c_peer, send_sem.at[a, base + 3 * line + s], c_sem.at[a, s])
            if 1 <= s <= line:
                j = s - 1
                wait(a, at, j, 1, p_sem.at[a, j])
                there = at(j, 1)
                push(there, there, second, send_sem.at[a, base + 2 * line + j], q_sem.at[a, line + j])
                push(there, there, c_peer, send_sem.at[a, base + 4 * line + j], c_sem.at[a, line + j])
                wait(a, at, j, 2, q_sem.at[a, j])
                there = at(j, 2)
                push(there, there, c_peer, send_sem.at[a, base + 5 * line + j], c_sem.at[a, 2 * line + j])
            if s >= 2:
                j = s - 2
                wait(a, at, j, 3, q_sem.at[a, line + j])
                there = at(j, 3)
                push(there, there, c_peer, send_sem.at[a, base + 6 * line + j], c_sem.at[a, 3 * line + j])
    for s in range(1, groups):
        peer = lax.rem(e - s + groups, groups)
        here = w_ref.at[pl.ds(pl.multiple_of(peer * rows, rows), rows), :]
        pltpu.make_async_remote_copy(
            src_ref=here, dst_ref=here, send_sem=tab_send.at[s], recv_sem=tab_recv.at[s],
            device_id=c_peer, device_id_type=MESH,
        ).wait_recv()
    for a, src, out, first, second, at in arrays:
        for kind in range(4):
            for j in range(line):
                flips = (kind % 2, kind // 2) if a == 0 else (kind // 2, kind % 2)
                here = slot(
                    out, lax.rem(z - j + line, line),
                    1 - y if flips[0] else y, 1 - x if flips[1] else x, 1 - c,
                )
                pltpu.make_async_remote_copy(
                    src_ref=here, dst_ref=here, send_sem=own_sem.at[a],
                    recv_sem=c_sem.at[a, kind * line + j], device_id=c_peer, device_id_type=MESH,
                ).wait_recv()
    for own in owns:
        own.wait()
    for copy in sends:
        copy.wait_send()


def gather_fast(tokens, cotangent, table, groups, halves):
    rows, quarter = tokens.shape
    line = groups // 2
    padded = jnp.pad(table, ((0, 0), (0, -table.shape[1] % LANES)))
    full = jax.ShapeDtypeStruct((groups * rows, halves * quarter), tokens.dtype)
    dma = pltpu.SemaphoreType.DMA
    return pl.pallas_call(
        functools.partial(gather_kernel, groups),
        out_shape=(full, full, jax.ShapeDtypeStruct((groups * rows, padded.shape[1]), table.dtype)),
        in_specs=[pl.BlockSpec(memory_space=pltpu.VMEM)] * 3,
        out_specs=[pl.BlockSpec(memory_space=pl.ANY)] * 3,
        scratch_shapes=[
            dma((2, 8 * line)), dma((2, line)), dma((2, line)), dma((2, 2 * line)),
            dma((2, 4 * line)), dma((groups,)), dma((groups,)), dma((3,)),
        ],
        compiler_params=pltpu.CompilerParams(collective_id=0, has_side_effects=True),
    )(tokens, cotangent, padded)


def scatter_kernel(
    groups, part, out_ref, core, one_a, one_b, two_a, two_b, last, send_sem, recv_sem,
):
    line = groups // 2
    z, y, x, c = place(groups)
    e, h = 2 * z + y, 2 * x + c
    wide = out_ref.shape[1] // 2
    f32 = jnp.float32
    y_peer = (2 * z + 1 - y, h)
    x_peer = (e, 2 * (1 - x) + c)
    c_peer = (e, 2 * x + 1 - c)
    others = [(2 * lax.rem(z + s, line) + y, h) for s in range(1, line)]
    greet(others + [y_peer, x_peer, c_peer])

    def col(xx, cc, side):
        return pl.ds(pl.multiple_of((2 * xx + cc) * 2 * wide + side * wide, wide), wide)

    def push(src, dst, peer, number):
        copy = pltpu.make_async_remote_copy(
            src_ref=src, dst_ref=dst, send_sem=send_sem.at[number], recv_sem=recv_sem.at[number],
            device_id=peer, device_id_type=MESH,
        )
        copy.start()
        return copy

    def add(dst, src):
        dst[...] = (dst[...].astype(f32) + src[...].astype(f32)).astype(dst.dtype)

    copies = []
    order = ((0, 0), (1, 0), (1, 1), (0, 1))
    for number, (side, keep) in enumerate(order):
        xx = x if keep else 1 - x
        copies.append(
            push(part.at[:, :, :, col(xx, 1 - c, side)], core.at[side, keep], c_peer, number)
        )

    def settle(number):
        side, keep = order[number]
        copies[number].wait_recv()
        xx = x if keep else 1 - x

        @pl.loop(0, line)
        def _(i):
            for j in range(2):
                add(core.at[side, keep, i, j], part.at[i, j, :, col(xx, c, side)])

    settle(0)
    a1 = push(core.at[0, 0], one_a, x_peer, 4)
    settle(1)
    settle(2)
    b1 = push(core.at[1, :, :, 1 - y], one_b, y_peer, 5)
    settle(3)
    a1.wait_recv()

    @pl.loop(0, line)
    def _(i):
        for j in range(2):
            add(one_a.at[i, j], core.at[0, 1, i, j])

    a2 = push(one_a.at[:, 1 - y], two_a, y_peer, 6)
    b1.wait_recv()

    @pl.loop(0, line)
    def _(i):
        for j in range(2):
            add(one_b.at[j, i], core.at[1, j, i, y])

    b2 = push(one_b.at[0], two_b, x_peer, 7)
    copies += [a1, b1, a2, b2]
    tails = ([], [])
    for side, copy, two in ((0, a2, two_a), (1, b2, two_b)):
        copy.wait_recv()

        @pl.loop(0, line)
        def _(i):
            add(two.at[i], one_a.at[i, y] if side == 0 else one_b.at[1, i])

        for s in range(1, line):
            number = 8 + side * line + s
            tails[side].append(
                push(two.at[lax.rem(z + s, line)], last.at[side, s - 1], others[s - 1], number)
            )
    for side, two in ((0, two_a), (1, two_b)):
        total = two[z].astype(f32)
        for s, copy in enumerate(tails[side]):
            copy.wait_recv()
            total = total + last[side, s].astype(f32)
        out_ref[:, side * wide:(side + 1) * wide] = total.astype(out_ref.dtype)
    for copy in copies + tails[0] + tails[1]:
        copy.wait_send()


def scatter_fast(part, groups, halves, rows, quarter):
    line = groups // 2
    wide = quarter // 2
    b16 = part.dtype
    dma = pltpu.SemaphoreType.DMA
    return pl.pallas_call(
        functools.partial(scatter_kernel, groups),
        out_shape=jax.ShapeDtypeStruct((rows, quarter), b16),
        in_specs=[pl.BlockSpec(memory_space=pltpu.VMEM)],
        out_specs=pl.BlockSpec(memory_space=pltpu.VMEM),
        scratch_shapes=[
            pltpu.VMEM((2, 2, line, 2, rows, wide), b16),
            pltpu.VMEM((line, 2, rows, wide), b16),
            pltpu.VMEM((2, line, rows, wide), b16),
            pltpu.VMEM((line, rows, wide), b16),
            pltpu.VMEM((line, rows, wide), b16),
            pltpu.VMEM((2, line - 1, rows, wide), b16),
            dma((8 + 2 * line,)),
            dma((8 + 2 * line,)),
        ],
        compiler_params=pltpu.CompilerParams(collective_id=1, has_side_effects=True),
    )(part.reshape(line, 2, rows, halves * quarter))


def per_device(tokens, cotangent, route, prob, w_gate, w_up, w_down):
    tok_rows, quarter = tokens.shape
    local_exp, units, width = w_gate.shape
    groups = lax.axis_size("expert")
    halves = lax.axis_size("half")
    experts = local_exp * groups
    total = groups * tok_rows
    f32 = jnp.float32
    me = lax.axis_index("expert")

    hit = route[:, :, None] == jnp.arange(experts, dtype=route.dtype)
    table = jnp.sum(jnp.where(hit, prob[:, :, None], 0).astype(f32), axis=1).astype(prob.dtype)
    fast = (
        groups > 2 and groups % 2 == 0 and halves == 2 * 2
        and tok_rows % 16 == 0 and quarter % (2 * LANES) == 0
        and total * width * 2 <= (1 << 23)
    )
    if fast:
        x, d, mine = gather_fast(tokens, cotangent, table, groups, halves)
        mine = lax.dynamic_slice_in_dim(mine, me * local_exp, local_exp, axis=1)
    else:
        mine = lax.all_to_all(
            table.reshape(tok_rows, groups, local_exp), "expert",
            split_axis=1, concat_axis=0, tiled=True,
        ).reshape(total, local_exp)
        x = gather_all(tokens, groups, halves)
        d = gather_all(cotangent, groups, halves)
    weight = jnp.repeat(mine.astype(f32), units, axis=1)

    wg = w_gate.reshape(local_exp * units, width)
    wu = w_up.reshape(local_exp * units, width)
    wd = w_down.reshape(local_exp * units, width)
    nt = (((1,), (1,)), ((), ()))
    tn = (((0,), (0,)), ((), ()))
    gate = lax.dot_general(x, wg, nt, preferred_element_type=f32)
    upval = lax.dot_general(x, wu, nt, preferred_element_type=f32)
    raw = lax.dot_general(d, wd, nt, preferred_element_type=f32)
    sig = jax.nn.sigmoid(gate)
    act = gate * sig
    hidden = act * upval
    score = jnp.sum((hidden * raw).reshape(total, local_exp, units), axis=2)
    dact = weight * raw
    hp = (weight * hidden).astype(jnp.bfloat16)
    dgate = (dact * upval * sig * (1.0 + gate * (1.0 - sig))).astype(jnp.bfloat16)
    dup = (dact * act).astype(jnp.bfloat16)
    part = lax.dot_general(
        jnp.concatenate([dgate, dup], axis=1), jnp.concatenate([wg, wu], axis=0),
        (((1,), (0,)), ((), ())), preferred_element_type=f32,
    ).astype(jnp.bfloat16)
    if fast:
        grad_tokens = scatter_fast(part, groups, halves, tok_rows, quarter)
    else:
        part = part.reshape(groups, tok_rows, halves, quarter).transpose(0, 2, 1, 3)
        grad_tokens = lax.psum_scatter(
            part.reshape(groups * halves * tok_rows, quarter), BOTH,
            scatter_dimension=0, tiled=True,
        )
    sent = jnp.broadcast_to(
        score.reshape(groups, 1, tok_rows, local_exp), (groups, halves, tok_rows, local_exp)
    ).reshape(groups * halves, tok_rows * local_exp)
    back = lax.all_to_all(sent, BOTH, split_axis=0, concat_axis=0, tiled=True)
    back = jnp.sum(back.reshape(groups, halves, tok_rows, local_exp), axis=1)
    back = back.transpose(1, 0, 2).reshape(tok_rows, 1, experts)
    grad_prob = jnp.sum(jnp.where(hit, back, 0), axis=2)
    shape = (local_exp, units, width)
    grad_gate = lax.dot_general(dgate, x, tn, preferred_element_type=f32).astype(jnp.bfloat16)
    grad_up = lax.dot_general(dup, x, tn, preferred_element_type=f32).astype(jnp.bfloat16)
    grad_down = lax.dot_general(hp, d, tn, preferred_element_type=f32).astype(jnp.bfloat16)
    return (
        grad_tokens,
        grad_prob,
        grad_gate.reshape(shape),
        grad_up.reshape(shape),
        grad_down.reshape(shape),
    )


def solution(mesh):
    in_specs = (
        P("expert", "half"),
        P("expert", "half"),
        P("expert", None),
        P("expert", None),
        P("expert", "half", None),
        P("expert", "half", None),
        P("expert", "half", None),
    )
    out_specs = (
        P("expert", "half"),
        P("expert", None),
        P("expert", "half", None),
        P("expert", "half", None),
        P("expert", "half", None),
    )
    return jax.shard_map(
        per_device, mesh=mesh, in_specs=in_specs, out_specs=out_specs, check_vma=False
    )
```

```python
import functools

import jax
import jax.numpy as jnp
from jax import lax
from jax.experimental import pallas as pl
from jax.experimental.pallas import tpu as pltpu
from jax.sharding import PartitionSpec as P

BOTH = ("expert", "half")


def gather_all(block, groups, halves):
    rows, quarter = block.shape
    parts = lax.all_gather(block, BOTH, axis=0).reshape(groups, halves, rows, quarter)
    return parts.transpose(0, 2, 1, 3).reshape(groups * rows, halves * quarter)


LANES = 128
MESH = pl.DeviceIdType.MESH


def place(groups):
    e, h = lax.axis_index("expert"), lax.axis_index("half")
    return lax.div(e, 2), lax.rem(e, 2), lax.div(h, 2), lax.rem(h, 2)


def across(z, step):
    bit = 1
    while bit <= step:
        if step & bit:
            z = z + bit * (1 - 2 * lax.rem(lax.div(z, bit), 2))
        bit *= 2
    return z


def greet(peers):
    barrier = pltpu.get_barrier_semaphore()
    for peer in peers:
        pl.semaphore_signal(barrier, inc=1, device_id=peer, device_id_type=MESH)
    pl.semaphore_wait(barrier, len(peers))


def gather_kernel(
    groups, tok_ref, cot_ref, tab_ref, x_ref, d_ref, w_ref,
    send_sem, z_sem, p_sem, q_sem, c_sem, tab_send, tab_recv, own_sem,
):
    line = groups // 2
    z, y, x, c = place(groups)
    e, h = 2 * z + y, 2 * x + c
    rows, quarter = tok_ref.shape
    y_peer = (2 * z + 1 - y, h)
    x_peer = (e, 2 * (1 - x) + c)
    c_peer = (e, 2 * x + 1 - c)
    ring = [(lax.rem(e + s, groups), h) for s in range(1, groups)]
    greet(ring + [x_peer, c_peer])

    sends, owns = [], []

    def push(src, dst, peer, number, sem):
        copy = pltpu.make_async_remote_copy(
            src_ref=src, dst_ref=dst, send_sem=number, recv_sem=sem,
            device_id=peer, device_id_type=MESH,
        )
        copy.start()
        sends.append(copy)

    def slot(out, zz, yy, xx, cc):
        row = pl.multiple_of((2 * zz + yy) * rows, rows)
        col = pl.multiple_of((2 * xx + cc) * quarter, quarter)
        return out.at[pl.ds(row, rows), pl.ds(col, quarter)]

    arrays = []
    for a, (src, out) in enumerate(((tok_ref, x_ref), (cot_ref, d_ref))):
        first, second = (y_peer, x_peer) if a == 0 else (x_peer, y_peer)

        def at(step, kind, out=out, a=a):
            zz = across(z, step)
            flip_first, flip_second = kind % 2, kind // 2
            fy, fx = (flip_first, flip_second) if a == 0 else (flip_second, flip_first)
            return slot(out, zz, 1 - y if fy else y, 1 - x if fx else x, c)

        arrays.append((a, src, out, first, second, at))

    def wait(a, at, step, kind, sem):
        here = at(step, kind)
        pltpu.make_async_remote_copy(
            src_ref=here, dst_ref=here, send_sem=own_sem.at[a], recv_sem=sem,
            device_id=c_peer, device_id_type=MESH,
        ).wait_recv()

    for a, src, out, first, second, at in arrays:
        here = slot(out, z, y, x, c)
        for s in range(1, line):
            push(src, here, (2 * across(z, s) + y, h), send_sem.at[a, s - 1], z_sem.at[a, s])
        own = pltpu.make_async_copy(src, here, own_sem.at[a])
        own.start()
        owns.append(own)
    for s in range(1, groups):
        here = w_ref.at[pl.ds(pl.multiple_of(e * rows, rows), rows), :]
        push(tab_ref, here, ring[s - 1], tab_send.at[s], tab_recv.at[s])
    own = pltpu.make_async_copy(
        tab_ref, w_ref.at[pl.ds(pl.multiple_of(e * rows, rows), rows), :], own_sem.at[2]
    )
    own.start()
    owns.append(own)

    base = line - 1
    for s in range(line + 2):
        for a, src, out, first, second, at in arrays:
            if s < line:
                if s > 0:
                    wait(a, at, s, 0, z_sem.at[a, s])
                there = at(s, 0)
                have = src if s == 0 else there
                push(have, there, first, send_sem.at[a, base + s], p_sem.at[a, s])
                push(have, there, second, send_sem.at[a, base + line + s], q_sem.at[a, s])
                push(have, there, c_peer, send_sem.at[a, base + 3 * line + s], c_sem.at[a, s])
            if 1 <= s <= line:
                j = s - 1
                wait(a, at, j, 1, p_sem.at[a, j])
                there = at(j, 1)
                push(there, there, second, send_sem.at[a, base + 2 * line + j], q_sem.at[a, line + j])
                push(there, there, c_peer, send_sem.at[a, base + 4 * line + j], c_sem.at[a, line + j])
                wait(a, at, j, 2, q_sem.at[a, j])
                there = at(j, 2)
                push(there, there, c_peer, send_sem.at[a, base + 5 * line + j], c_sem.at[a, 2 * line + j])
            if s >= 2:
                j = s - 2
                wait(a, at, j, 3, q_sem.at[a, line + j])
                there = at(j, 3)
                push(there, there, c_peer, send_sem.at[a, base + 6 * line + j], c_sem.at[a, 3 * line + j])
    for s in range(1, groups):
        peer = lax.rem(e - s + groups, groups)
        here = w_ref.at[pl.ds(pl.multiple_of(peer * rows, rows), rows), :]
        pltpu.make_async_remote_copy(
            src_ref=here, dst_ref=here, send_sem=tab_send.at[s], recv_sem=tab_recv.at[s],
            device_id=c_peer, device_id_type=MESH,
        ).wait_recv()
    for a, src, out, first, second, at in arrays:
        for kind in range(4):
            for j in range(line):
                flips = (kind % 2, kind // 2) if a == 0 else (kind // 2, kind % 2)
                here = slot(
                    out, across(z, j),
                    1 - y if flips[0] else y, 1 - x if flips[1] else x, 1 - c,
                )
                pltpu.make_async_remote_copy(
                    src_ref=here, dst_ref=here, send_sem=own_sem.at[a],
                    recv_sem=c_sem.at[a, kind * line + j], device_id=c_peer, device_id_type=MESH,
                ).wait_recv()
    for own in owns:
        own.wait()
    for copy in sends:
        copy.wait_send()


def gather_fast(tokens, cotangent, table, groups, halves):
    rows, quarter = tokens.shape
    line = groups // 2
    padded = jnp.pad(table, ((0, 0), (0, -table.shape[1] % LANES)))
    full = jax.ShapeDtypeStruct((groups * rows, halves * quarter), tokens.dtype)
    dma = pltpu.SemaphoreType.DMA
    return pl.pallas_call(
        functools.partial(gather_kernel, groups),
        out_shape=(full, full, jax.ShapeDtypeStruct((groups * rows, padded.shape[1]), table.dtype)),
        in_specs=[pl.BlockSpec(memory_space=pltpu.VMEM)] * 3,
        out_specs=[pl.BlockSpec(memory_space=pl.ANY)] * 3,
        scratch_shapes=[
            dma((2, 8 * line)), dma((2, line)), dma((2, line)), dma((2, 2 * line)),
            dma((2, 4 * line)), dma((groups,)), dma((groups,)), dma((3,)),
        ],
        compiler_params=pltpu.CompilerParams(collective_id=0, has_side_effects=True),
    )(tokens, cotangent, padded)


def scatter_kernel(
    groups, halves, part, score, out_ref, back_ref, core, one_a, one_b, two_a, two_b, last,
    send_sem, recv_sem, score_send, score_recv, own_sem,
):
    line = groups // 2
    z, y, x, c = place(groups)
    e, h = 2 * z + y, 2 * x + c
    wide = out_ref.shape[1] // 2
    f32 = jnp.float32
    y_peer = (2 * z + 1 - y, h)
    x_peer = (e, 2 * (1 - x) + c)
    c_peer = (e, 2 * x + 1 - c)
    others = [(2 * lax.rem(z + s, line) + y, h) for s in range(1, line)]
    peers = [
        (lax.rem(e + i, groups), lax.rem(h + j, halves))
        for i in range(groups) for j in range(halves) if i + j
    ]
    greet(peers)

    def col(xx, cc, side):
        return pl.ds(pl.multiple_of((2 * xx + cc) * 2 * wide + side * wide, wide), wide)

    def push(src, dst, peer, number):
        copy = pltpu.make_async_remote_copy(
            src_ref=src, dst_ref=dst, send_sem=send_sem.at[number], recv_sem=recv_sem.at[number],
            device_id=peer, device_id_type=MESH,
        )
        copy.start()
        return copy

    def add(dst, src):
        dst[...] = (dst[...].astype(f32) + src[...].astype(f32)).astype(dst.dtype)

    copies = []
    order = ((0, 0), (1, 0), (1, 1), (0, 1))
    scores = []
    mine = e * halves + h

    def send_scores():
        for number, peer in enumerate(peers):
            copy = pltpu.make_async_remote_copy(
                src_ref=score.at[peer[0]], dst_ref=back_ref.at[mine],
                send_sem=score_send.at[number], recv_sem=score_recv.at[number],
                device_id=peer, device_id_type=MESH,
            )
            copy.start()
            scores.append(copy)

    own = pltpu.make_async_copy(score.at[e], back_ref.at[mine], own_sem.at[0])
    own.start()
    for number, (side, keep) in enumerate(order):
        xx = x if keep else 1 - x
        copies.append(
            push(part.at[:, :, :, col(xx, 1 - c, side)], core.at[side, keep], c_peer, number)
        )

    def settle(number):
        side, keep = order[number]
        copies[number].wait_recv()
        xx = x if keep else 1 - x

        @pl.loop(0, line)
        def _(i):
            for j in range(2):
                add(core.at[side, keep, i, j], part.at[i, j, :, col(xx, c, side)])

    settle(0)
    a1 = push(core.at[0, 0], one_a, x_peer, 4)
    settle(1)
    settle(2)
    b1 = push(core.at[1, :, :, 1 - y], one_b, y_peer, 5)
    send_scores()
    settle(3)
    a1.wait_recv()

    @pl.loop(0, line)
    def _(i):
        for j in range(2):
            add(one_a.at[i, j], core.at[0, 1, i, j])

    a2 = push(one_a.at[:, 1 - y], two_a, y_peer, 6)
    b1.wait_recv()

    @pl.loop(0, line)
    def _(i):
        for j in range(2):
            add(one_b.at[j, i], core.at[1, j, i, y])

    b2 = push(one_b.at[0], two_b, x_peer, 7)
    copies += [a1, b1, a2, b2]
    tails = ([], [])
    for side, copy, two in ((0, a2, two_a), (1, b2, two_b)):
        copy.wait_recv()

        @pl.loop(0, line)
        def _(i):
            add(two.at[i], one_a.at[i, y] if side == 0 else one_b.at[1, i])

        for s in range(1, line):
            number = 8 + side * line + s
            tails[side].append(
                push(two.at[lax.rem(z + s, line)], last.at[side, s - 1], others[s - 1], number)
            )
    for side, two in ((0, two_a), (1, two_b)):
        total = two[z].astype(f32)
        for s, copy in enumerate(tails[side]):
            copy.wait_recv()
            total = total + last[side, s].astype(f32)
        out_ref[:, side * wide:(side + 1) * wide] = total.astype(out_ref.dtype)
    for copy in scores:
        copy.wait_recv()
    own.wait()
    for copy in copies + tails[0] + tails[1] + scores:
        copy.wait_send()


def scatter_fast(part, score, groups, halves, rows, quarter):
    line = groups // 2
    wide = quarter // 2
    b16 = part.dtype
    dma = pltpu.SemaphoreType.DMA
    return pl.pallas_call(
        functools.partial(scatter_kernel, groups, halves),
        out_shape=(
            jax.ShapeDtypeStruct((rows, quarter), b16),
            jax.ShapeDtypeStruct((groups * halves,) + score.shape[1:], score.dtype),
        ),
        in_specs=[pl.BlockSpec(memory_space=pltpu.VMEM)] * 2,
        out_specs=[pl.BlockSpec(memory_space=pltpu.VMEM)] * 2,
        scratch_shapes=[
            pltpu.VMEM((2, 2, line, 2, rows, wide), b16),
            pltpu.VMEM((line, 2, rows, wide), b16),
            pltpu.VMEM((2, line, rows, wide), b16),
            pltpu.VMEM((line, rows, wide), b16),
            pltpu.VMEM((line, rows, wide), b16),
            pltpu.VMEM((2, line - 1, rows, wide), b16),
            dma((8 + 2 * line,)),
            dma((8 + 2 * line,)),
            dma((groups * halves - 1,)),
            dma((groups * halves - 1,)),
            dma((1,)),
        ],
        compiler_params=pltpu.CompilerParams(collective_id=1, has_side_effects=True),
    )(part.reshape(line, 2, rows, halves * quarter), score)


def per_device(tokens, cotangent, route, prob, w_gate, w_up, w_down):
    tok_rows, quarter = tokens.shape
    local_exp, units, width = w_gate.shape
    groups = lax.axis_size("expert")
    halves = lax.axis_size("half")
    experts = local_exp * groups
    total = groups * tok_rows
    f32 = jnp.float32
    me = lax.axis_index("expert")

    hit = route[:, :, None] == jnp.arange(experts, dtype=route.dtype)
    table = jnp.sum(jnp.where(hit, prob[:, :, None], 0).astype(f32), axis=1).astype(prob.dtype)
    fast = (
        groups > 2 and groups & (groups - 1) == 0 and halves == 2 * 2
        and tok_rows % LANES == 0 and quarter % (2 * LANES) == 0
        and total * width * 2 <= (1 << 23)
    )
    if fast:
        x, d, mine = gather_fast(tokens, cotangent, table, groups, halves)
        mine = lax.dynamic_slice_in_dim(mine, me * local_exp, local_exp, axis=1)
    else:
        mine = lax.all_to_all(
            table.reshape(tok_rows, groups, local_exp), "expert",
            split_axis=1, concat_axis=0, tiled=True,
        ).reshape(total, local_exp)
        x = gather_all(tokens, groups, halves)
        d = gather_all(cotangent, groups, halves)
    weight = jnp.repeat(mine.astype(f32), units, axis=1)

    wg = w_gate.reshape(local_exp * units, width)
    wu = w_up.reshape(local_exp * units, width)
    wd = w_down.reshape(local_exp * units, width)
    nt = (((1,), (1,)), ((), ()))
    tn = (((0,), (0,)), ((), ()))
    gate = lax.dot_general(x, wg, nt, preferred_element_type=f32)
    upval = lax.dot_general(x, wu, nt, preferred_element_type=f32)
    raw = lax.dot_general(d, wd, nt, preferred_element_type=f32)
    sig = jax.nn.sigmoid(gate)
    act = gate * sig
    hidden = act * upval
    score = jnp.sum((hidden * raw).reshape(total, local_exp, units), axis=2)
    dact = weight * raw
    hp = (weight * hidden).astype(jnp.bfloat16)
    dgate = (dact * upval * sig * (1.0 + gate * (1.0 - sig))).astype(jnp.bfloat16)
    dup = (dact * act).astype(jnp.bfloat16)
    part = lax.dot_general(
        jnp.concatenate([dgate, dup], axis=1), jnp.concatenate([wg, wu], axis=0),
        (((1,), (0,)), ((), ())), preferred_element_type=f32,
    ).astype(jnp.bfloat16)
    if fast:
        by_group = score.reshape(groups, tok_rows, local_exp).transpose(0, 2, 1)
        by_group = jnp.pad(by_group, ((0, 0), (0, -local_exp % 8), (0, 0)))
        grad_tokens, back = scatter_fast(part, by_group, groups, halves, tok_rows, quarter)
        back = back[:, :local_exp].reshape(groups, halves, local_exp, tok_rows)
        back = jnp.sum(back, axis=1).transpose(2, 0, 1).reshape(tok_rows, 1, experts)
    else:
        part = part.reshape(groups, tok_rows, halves, quarter).transpose(0, 2, 1, 3)
        grad_tokens = lax.psum_scatter(
            part.reshape(groups * halves * tok_rows, quarter), BOTH,
            scatter_dimension=0, tiled=True,
        )
        sent = jnp.broadcast_to(
            score.reshape(groups, 1, tok_rows, local_exp), (groups, halves, tok_rows, local_exp)
        ).reshape(groups * halves, tok_rows * local_exp)
        back = lax.all_to_all(sent, BOTH, split_axis=0, concat_axis=0, tiled=True)
        back = jnp.sum(back.reshape(groups, halves, tok_rows, local_exp), axis=1)
        back = back.transpose(1, 0, 2).reshape(tok_rows, 1, experts)
    grad_prob = jnp.sum(jnp.where(hit, back, 0), axis=2)
    shape = (local_exp, units, width)
    grad_gate = lax.dot_general(dgate, x, tn, preferred_element_type=f32).astype(jnp.bfloat16)
    grad_up = lax.dot_general(dup, x, tn, preferred_element_type=f32).astype(jnp.bfloat16)
    grad_down = lax.dot_general(hp, d, tn, preferred_element_type=f32).astype(jnp.bfloat16)
    return (
        grad_tokens,
        grad_prob,
        grad_gate.reshape(shape),
        grad_up.reshape(shape),
        grad_down.reshape(shape),
    )


def solution(mesh):
    in_specs = (
        P("expert", "half"),
        P("expert", "half"),
        P("expert", None),
        P("expert", None),
        P("expert", "half", None),
        P("expert", "half", None),
        P("expert", "half", None),
    )
    out_specs = (
        P("expert", "half"),
        P("expert", None),
        P("expert", "half", None),
        P("expert", "half", None),
        P("expert", "half", None),
    )
    return jax.shard_map(
        per_device, mesh=mesh, in_specs=in_specs, out_specs=out_specs, check_vma=False
    )
```
